32 devices in a mesh: groups: 2 (over y), dp: 4 (over z), section: 2 (over x), tensor: 2 (over core).
Axes of the slice: x: 2, y: 2, z: 4, core: 2. Of those that a mesh axis runs over, the one named last changes fastest.
Arguments:
- hidden: bfloat16 [128, 8, 5120], P(('groups', 'dp')), parts along dimension 0, may hold values from -6 to 6
- unembed: bfloat16 [128, 8, 5120], P(('groups', 'dp')), parts along dimension 0, may hold values from -0.02734375 to 0.02734375
- value_proj: bfloat16 [2, 5120, 512], P('section', 'dp', 'tensor'), may hold values from -0.078125 to 0.078125
- output_proj: bfloat16 [2, 512, 5120], P('section', 'tensor', 'dp'), may hold values from -0.125 to 0.125
- norm_gains: float32 [2, 5120], P('section'), may hold values from 0.1 to 1.9
- survive: int32 [8], P(('groups', 'dp')), parts along dimension 0, may hold values from 0 to 1, as said below
- lengths: int32 [128], P(('groups', 'dp')), parts along dimension 0, may hold values from 1 to 8
- assign: int32 [128], P(('groups', 'dp')), parts along dimension 0, may hold values from 0 to 16, as said below
- advantage: float32 [128], P(('groups', 'dp')), parts along dimension 0, may hold values from -4 to 4
- reference_logit: float32 [128, 8], P(('groups', 'dp')), parts along dimension 0, may hold values from -4 to 4
- recorded_gap: float32 [128, 8], P(('groups', 'dp')), parts along dimension 0, may hold values from -2 to 2
Outputs:
- grad_value: float32 [4, 5120, 512], P(('groups', 'section'), 'dp', 'tensor'), parts along dimension 0
- grad_output: float32 [4, 512, 5120], P(('groups', 'section'), 'tensor', 'dp'), parts along dimension 0
The draws below stay inside these ranges and needn't reach their ends.
There are 2 independent parts, one for each index of `groups`. The reference program is written for one: setup_inputs(seed, part) draws one part's arguments, and reference() takes and returns one part's arrays. A program takes and returns all parts, laid end to end along the dimension named above; an argument that names none is the same for every part. Nothing has to cross between parts.
Inputs may be any that keep to these rules, and one draw needn't show every extreme that they name: `survive`: 1 where the group of 16 responses is kept, 0 where it is dropped; in every draw all groups of some dp index are kept. `assign`: the 16 slots of a dp index list the local positions (0 to 15) of the responses of its kept groups, each exactly once, then hold 16 in every other slot.
All inputs are finite; a program needn't handle non-finite values.
Results may differ from the reference program's by a relative error of at most 0.029.
Values may be sent and summed in bfloat16 or wider, within the bound.
A program may use at most 64 MiB of HBM per device.

```python
import math
import jax
import jax.numpy as jnp
from jax import lax

D = 5120
VALUE_W = 512
GROUP = 16
GROUPS_DEV = 1
LMAX = 8
LAYERS = 2
RESP_DEV = 16
RESPONSES = 64
GROUPS = 4
N_DP = 4
N_TENSOR = 2


def survival_plan(key):
    base = jax.random.fold_in(key, 17)
    roll_key, force_key, order_key = jax.random.split(base, 3)
    device = jnp.arange(GROUPS, dtype=jnp.int32) // GROUPS_DEV
    threshold = 300 + 700 * device // max(N_DP - 1, 1)
    survival_roll = jax.random.randint(roll_key, (GROUPS,), 0, 1000)
    forced = jax.random.randint(force_key, (), 0, N_DP)
    alive_mask = ((survival_roll < threshold) | (device == forced)).astype(jnp.int32)
    return (alive_mask, order_key)


def draw_survive(key, part):
    alive_mask, order_key = survival_plan(key)
    return alive_mask


def draw_assign(key, part):
    alive_mask, order_key = survival_plan(key)
    per_device = jnp.repeat(alive_mask, GROUP).reshape(N_DP, RESP_DEV)
    subkeys = jax.random.split(order_key, N_DP)
    priority = jax.vmap(lambda subkey: jax.random.permutation(subkey, RESP_DEV))(subkeys).astype(jnp.int32)
    sort_key = (1 - per_device) * RESP_DEV + priority
    slot_order = jnp.argsort(sort_key, axis=1, stable=True).astype(jnp.int32)
    alive_count = jnp.sum(per_device, axis=1, keepdims=True)
    slot_index = lax.broadcasted_iota(jnp.int32, (N_DP, RESP_DEV), 1)
    return jnp.where(slot_index < alive_count, slot_order, RESP_DEV).astype(jnp.int32).reshape(RESPONSES)


def set_ends(drawn, rng, low, high):
    extent = drawn.shape
    spot = [jax.random.randint(jax.random.fold_in(rng, axis), (), 0, extent[axis]) for axis in range(len(extent))]
    drawn = drawn.at[tuple(spot)].set(low)
    longest = extent.index(max(extent))
    spot[longest] = (spot[longest] + 1) % extent[longest]
    return drawn.at[tuple(spot)].set(high)


def with_spikes(values, rng, source, target, parts, factor):
    owner, partner = [(jnp.arange(values.shape[axis_at]) // (values.shape[axis_at] // parts)).reshape([-1 if axis == axis_at else 1 for axis in range(values.ndim)]) for axis_at in (source, target)]
    chosen = jax.random.permutation(rng, parts)[partner]
    strong = (owner == chosen) | (owner == (partner + parts // 2) % parts)
    return jnp.where(strong, factor * values, values)


def shard_levels(own_key, shape, cuts, least, top_value):
    gain, own = 1.0, jax.random.fold_in(own_key, 6)
    for position, parts in cuts:
        heights = jnp.exp(jax.random.uniform(jax.random.fold_in(own, position), (parts,), jnp.float32, least / len(cuts), top_value / len(cuts)))
        gain = gain * jnp.repeat(heights, shape[position] // parts).reshape([-1 if axis == position else 1 for axis in range(len(shape))])
    return gain


def normal_values(own_key, dims, scale, limit, cuts=(), held_as=jnp.bfloat16):
    result = jax.random.normal(own_key, dims, jnp.float32) * scale
    if len(cuts) > 0:
        result = shard_levels(own_key, dims, cuts, -0.22, 0.18) * result
    return jnp.clip(result, min=-limit, max=limit).astype(held_as)


def heavy_noise(key, shape, scale, most, cuts, heavy, held_as=jnp.bfloat16):
    entries = scale * jax.random.normal(key, shape, jnp.float32)
    if cuts:
        entries = entries * shard_levels(key, shape, cuts, -0.22, 0.18)
    return jnp.clip(with_spikes(entries, jax.random.fold_in(key, 3), *heavy), -most, most).astype(held_as)


def setup_inputs(seed: int = 0, part: int = 0) -> dict:
    key_list = jax.random.split(jax.random.key(seed), 12)
    own_keys = jax.random.split(jax.random.fold_in(key_list[11], part), 12)
    return {
        "hidden": heavy_noise(own_keys[0], (RESPONSES, LMAX, D), 1.0, 6.0, ((0, 4),), (0, 2, 4, 2.0)),
        "unembed": normal_values(own_keys[1], (RESPONSES, LMAX, D), (10 * D) ** -0.5, 0.02734375, ((0, 4),)),
        "value_proj": normal_values(key_list[2], (LAYERS, D, VALUE_W), D ** -0.5, 0.078125, ((0, 2), (1, 4), (2, 2))),
        "output_proj": normal_values(key_list[3], (LAYERS, VALUE_W, D), (4 * VALUE_W) ** -0.5, 0.125, ((0, 2), (1, 2), (2, 4))),
        "norm_gains": jnp.clip(1.0 + 0.18 * jax.random.normal(key_list[4], (LAYERS, D), jnp.float32), 0.1, 1.9),
        "survive": draw_survive(jax.random.fold_in(jax.random.fold_in(key_list[11], part), 71), part),
        "lengths": set_ends(jax.random.randint(own_keys[6], (RESPONSES,), 1, LMAX + 1), jax.random.fold_in(own_keys[6], 1), 1, LMAX).astype(jnp.int32),
        "assign": draw_assign(jax.random.fold_in(jax.random.fold_in(key_list[11], part), 71), part),
        "advantage": normal_values(own_keys[8], (RESPONSES,), 1.0, 4.0, ((0, 4),), jnp.float32),
        "reference_logit": normal_values(own_keys[9], (RESPONSES, LMAX), 0.7, 4.0, ((0, 4),), jnp.float32),
        "recorded_gap": normal_values(own_keys[10], (RESPONSES, LMAX), 0.3, 2.0, ((0, 4),), jnp.float32),
    }


eps_norm = 1e-06
loss_scale = 4096.0
clip_high = math.log(1.28)
clip_low = math.log(0.8)

def norm_forward(row_block, norm_gain):
    values = row_block.astype(jnp.float32)
    inverse = lax.rsqrt(lax.optimization_barrier(jnp.mean(values * values, axis=-1, keepdims=True)) + eps_norm)
    return (values, inverse, (values * inverse * norm_gain).astype(jnp.bfloat16))

def norm_backward(values, inverse, norm_gain, upstream):
    scaled = upstream * norm_gain
    inner_sum = lax.optimization_barrier(jnp.sum(scaled * values, axis=-1, keepdims=True)) / values.shape[-1]
    return inverse * scaled - values * (inverse * inverse * inverse) * inner_sum

def contract_last(left_rows, right_rows):
    return lax.dot_general(left_rows, right_rows, (((1,), (1,)), ((), ())), preferred_element_type=jnp.float32)

def rounded(partial_piece):
    return lax.optimization_barrier(partial_piece.astype(jnp.bfloat16)).astype(jnp.float32)

def reference(hidden, unembed, value_proj, output_proj, norm_gains, survive, lengths, assign, advantage, reference_logit, recorded_gap):
    owner_index = jnp.arange(RESPONSES, dtype=jnp.int32) // RESP_DEV
    chosen = jnp.where(assign >= RESP_DEV, RESPONSES, assign + owner_index * RESP_DEV).astype(jnp.int32)

    def pick(array):
        return jnp.take(array, chosen, axis=0, mode='fill', fill_value=0)
    row_count = RESPONSES * LMAX
    block_width = VALUE_W // N_TENSOR
    current = pick(hidden).reshape(row_count, D)
    unembed_rows = pick(unembed).reshape(row_count, D).astype(jnp.float32)
    positions = lax.broadcasted_iota(jnp.int32, (RESPONSES, LMAX), 1)
    live_mask = (positions < pick(lengths)[:, None]).astype(jnp.float32)
    advantages = jnp.broadcast_to(pick(advantage)[:, None], (RESPONSES, LMAX))
    gap_rows = pick(recorded_gap)
    clipped = (advantages > 0) & (gap_rows > clip_high) | (advantages < 0) & (gap_rows < clip_low)
    kept_mask = 1.0 - clipped.astype(jnp.float32)
    alive_mask = jnp.repeat(survive, GROUP)
    token_count = jnp.sum((alive_mask * lengths).astype(jnp.float32))
    weight_rows = (-loss_scale * advantages * kept_mask * live_mask).reshape(row_count)
    logit_base = pick(reference_logit).reshape(row_count)
    saved = []
    for layer_index in range(LAYERS):
        values, inverse, normed = norm_forward(current, norm_gains[layer_index])
        projected = jnp.dot(normed, value_proj[layer_index], preferred_element_type=jnp.float32).astype(jnp.bfloat16)
        mixed_sum = jnp.zeros((row_count, D), jnp.float32)
        for tensor_part in range(N_TENSOR):
            low = tensor_part * block_width
            partial_piece = jnp.dot(projected[:, low:low + block_width], output_proj[layer_index, low:low + block_width, :], preferred_element_type=jnp.float32)
            mixed_sum = mixed_sum + rounded(partial_piece)
        saved.append((current, normed, projected))
        current = (values + mixed_sum).astype(jnp.bfloat16)
    top_rows = current.astype(jnp.float32)
    logit = lax.optimization_barrier(jnp.sum(top_rows * unembed_rows, axis=-1))
    seed_rows = weight_rows * jnp.exp(logit - logit_base)
    upstream = (seed_rows[:, None] * unembed_rows).astype(jnp.bfloat16)
    grads_value = [None] * LAYERS
    grads_output = [None] * LAYERS
    for layer_index in reversed(range(LAYERS)):
        entering, normed, projected = saved[layer_index]
        grad_projected = contract_last(upstream, output_proj[layer_index]).astype(jnp.bfloat16)
        grad_normed = jnp.zeros((row_count, D), jnp.float32)
        for tensor_part in range(N_TENSOR):
            low = tensor_part * block_width
            partial_piece = contract_last(grad_projected[:, low:low + block_width], value_proj[layer_index][:, low:low + block_width])
            grad_normed = grad_normed + rounded(partial_piece)
        grads_value[layer_index] = jnp.dot(normed.T, grad_projected, preferred_element_type=jnp.float32) / token_count
        grads_output[layer_index] = jnp.dot(projected.T, upstream, preferred_element_type=jnp.float32) / token_count
        values, inverse, unused_normed = norm_forward(entering, norm_gains[layer_index])
        upstream = (upstream.astype(jnp.float32) + norm_backward(values, inverse, norm_gains[layer_index], grad_normed)).astype(jnp.bfloat16)
    return (jnp.stack(grads_value), jnp.stack(grads_output))
```

```python
import functools
import math

import jax
import jax.numpy as jnp
from jax import lax
from jax.experimental import pallas as pl
from jax.experimental.pallas import tpu as pltpu
from jax.sharding import PartitionSpec as P

eps_norm = 1e-06
loss_scale = 4096.0
clip_high = math.log(1.28)
clip_low = math.log(0.8)
LANES = 128
KINDS = ("a", "xf", "uf", "p", "q", "pj", "pjf", "gq", "gqf", "sc", "tk", "x", "g", "w", "e")
BF = jnp.bfloat16
F32 = jnp.float32


def dot(a, b, ca=1, cb=0):
    return lax.dot_general(a, b, (((ca,), (cb,)), ((), ())), preferred_element_type=F32)


def halves(value):
    high = value.astype(BF)
    return high, (value - high.astype(F32)).astype(BF)


def kernel(
    n, sections, width,
    src, w1, w2, gain, rinfo, tok,
    dw1, dw2,
    xs, us, xg, pb, pr, qb, qr, pj, gq, sc, w1o, w2o, yx, yg, tk, exs, exr, pacc, qacc, rkeep,
    ss, rs,
):
    j = lax.axis_index("dp")
    s = lax.axis_index("section")
    t = lax.axis_index("tensor")
    o = 1 - t
    rows = src.shape[1]
    v = w1.shape[2]
    last = sections - 1
    partner = {"tensor": o}

    def blk(b):
        return pl.ds(pl.multiple_of(b * rows, rows), rows)

    def peer(k):
        return lax.rem(j + k, n)

    def send(kind, si, ri, a, b, dev):
        k = KINDS.index(kind)
        pltpu.make_async_remote_copy(
            src_ref=a, dst_ref=b, send_sem=ss.at[k, si], recv_sem=rs.at[k, ri],
            device_id=dev, device_id_type=pl.DeviceIdType.MESH,
        ).start()

    def handle(kind, i, a):
        k = KINDS.index(kind)
        return pltpu.make_async_remote_copy(
            src_ref=a, dst_ref=a, send_sem=ss.at[k, i], recv_sem=rs.at[k, i],
            device_id=partner, device_id_type=pl.DeviceIdType.MESH,
        )

    def got(kind, i, a):
        handle(kind, i, a).wait_recv()

    def sent(kind, i, a):
        handle(kind, i, a).wait_send()

    def others(body):
        def step(k, carry):
            body(peer(k))
            return carry
        lax.fori_loop(1, n, step, 0)

    def everyone(body):
        def step(k, carry):
            body(peer(k))
            return carry
        lax.fori_loop(0, n, step, 0)

    barrier = pltpu.get_barrier_semaphore()

    def greet(dev):
        pl.semaphore_signal(barrier, inc=1, device_id=dev, device_id_type=pl.DeviceIdType.MESH)

    for k in range(1, n):
        greet({"dp": peer(k)})
    greet(partner)

    @pl.when(s > 0)
    def _():
        greet({"section": s - 1})

    @pl.when(s < last)
    def _():
        greet({"section": s + 1})

    pl.semaphore_wait(barrier, n + jnp.where(s > 0, 1, 0) + jnp.where(s < last, 1, 0))

    def start_common():
        send("w", 0, 0, w1.at[o], w1o, partner)
        send("w", 1, 1, w2.at[o], w2o, partner)
        others(lambda b: send("tk", b, j, tok, tk.at[j], {"dp": b}))
        tk[j] = tok[...]

    def all_to_all(dst):
        others(lambda b: send("a", b, j, src.at[b * 2 + t], dst.at[t, blk(j)], {"dp": b}))
        dst[0, blk(j)] = src[j * 2]
        dst[1, blk(j)] = src[j * 2 + 1]

    def arrive(kind, fkind, buf, b):
        got(kind, b, buf.at[t, blk(b)])
        send(fkind, b, b, buf.at[t, blk(b)], buf.at[t, blk(b)], partner)
        got(fkind, b, buf.at[o, blk(b)])

    lane = lax.broadcasted_iota(jnp.int32, (rows, LANES), 1)

    def pack(values):
        packed = jnp.zeros((rows, LANES), F32)
        for i, value in enumerate(values):
            for half, part in enumerate(halves(value)):
                packed = jnp.where(lane == 2 * i + half, part.astype(F32), packed)
        return packed.astype(BF)

    def unpack(packed, i):
        return jnp.sum(
            jnp.where((lane == 2 * i) | (lane == 2 * i + 1), packed.astype(F32), 0.0),
            axis=1, keepdims=True,
        )

    def forward_chunk(b, with_logit):
        total = jnp.zeros((rows, v), F32)
        squares = jnp.zeros((rows, 1), F32)
        logit = jnp.zeros((rows, 1), F32)
        for h in range(2):
            x = xs[h, blk(b)].astype(F32)
            squares += jnp.sum(x * x, axis=1, keepdims=True)
            if with_logit:
                logit += jnp.sum(x * us[h, blk(b)].astype(F32), axis=1, keepdims=True)
            scaled = (x * gain[h]).astype(BF)
            xg[h, blk(b)] = scaled
            total += dot(scaled, w1[h])
        pb[blk(b), :v] = total.astype(BF)
        pb[blk(b), v:] = pack([squares, logit] if with_logit else [squares])

        @pl.when(b != j)
        def _():
            send("p", b, j, pb.at[blk(b)], pr.at[j], {"dp": b})

    def backward_chunk(b):
        total = dot(us[0, blk(b)], w2[0], 1, 1) + dot(us[1, blk(b)], w2[1], 1, 1)
        qb[blk(b)] = total.astype(BF)

        @pl.when(b != j)
        def _():
            send("q", b, j, qb.at[blk(b)], qr.at[j], {"dp": b})

    def reduce(kind, own, landed, acc):
        acc[...] = own[blk(j)].astype(F32)

        def add(b):
            got(kind, b, landed.at[b])
            acc[...] += landed[b].astype(F32)
        others(add)

    def share(kind, buf, forward):
        others(lambda b: send(kind, b, j, buf.at[t, blk(j)], buf.at[t, blk(j)], {"dp": b}))
        if forward:
            send(kind + "f", j, j, buf.at[t, blk(j)], buf.at[t, blk(j)], partner)

    def shared(kind, buf, b):
        @pl.when(b != j)
        def _():
            got(kind, b, buf.at[t, blk(b)])
            send(kind + "f", b, b, buf.at[t, blk(b)], buf.at[t, blk(b)], partner)
        got(kind + "f", b, buf.at[o, blk(b)])

    def own_inverse():
        inverse = lax.rsqrt(unpack(pacc[:, v:], 0) / width + eps_norm)
        rkeep[...] = jnp.broadcast_to(inverse, (rows, LANES))
        return inverse

    def forward_out():
        reduce("p", pb, pr, pacc)
        inverse = own_inverse()
        pj[t, blk(j)] = (inverse * pacc[:, :v]).astype(BF)
        share("pj", pj, True)
        got("w", 1, w2o)

        def chunk(b):
            shared("pj", pj, b)
            mixed = dot(pj[t, blk(b)], w2[t]) + dot(pj[o, blk(b)], w2o[...])
            yx[blk(b)] = (xs[t, blk(b)].astype(F32) + mixed).astype(BF)
            send("x", b, b, yx.at[blk(b)], xs.at[t, blk(b)], {"section": s + 1})
        everyone(chunk)

    def dot_over_units():
        exs[...] = jnp.broadcast_to(
            jnp.sum(pacc[:, :v] * qacc[...], axis=1, keepdims=True), (rows, LANES)
        )
        send("e", 0, 0, exs, exr, partner)
        got("e", 0, exr)
        return exs[:, :1] + exr[:, :1]

    def backward_out(is_last):
        reduce("q", qb, qr, qacc)
        inner = dot_over_units()
        inverse = rkeep[:, :1]
        if is_last:
            logit = unpack(pacc[:, v:], 1) + inverse * inner
            seed = rinfo[:, 0:1] * jnp.exp(logit - rinfo[:, 1:2])
            scale = seed * inverse
            pj[t, blk(j)] = (scale * pacc[:, :v]).astype(BF)
        else:
            seed = jnp.ones((rows, 1), F32)
            scale = inverse
        gq[t, blk(j)] = (scale * qacc[...]).astype(BF)
        sc[j] = pack([inverse * inverse * inverse * (seed * inner) / width, seed])
        share("gq", gq, True)
        others(lambda b: send("sc", b, j, sc.at[j], sc.at[j], {"dp": b}))
        if is_last:
            share("pj", pj, False)
        got("w", 0, w1o)

        def chunk(b):
            shared("gq", gq, b)

            @pl.when(b != j)
            def _():
                got("sc", b, sc.at[b])
            packed = sc[b]
            grad = dot(gq[t, blk(b)], w1[t], 1, 1) + dot(gq[o, blk(b)], w1o[...], 1, 1)
            upstream = us[t, blk(b)].astype(F32)
            if is_last:
                upstream = unpack(packed, 1) * upstream
            yg[blk(b)] = (
                upstream + gain[t] * grad - unpack(packed, 0) * xs[t, blk(b)].astype(F32)
            ).astype(BF)
            send("g", b, b, yg.at[blk(b)], us.at[t, blk(b)], {"section": s - 1})
        everyone(chunk)

    def tokens():
        count = tk[j]

        def add(b, total):
            return total
        others(lambda b: got("tk", b, tk.at[b]))
        count = tk[0]
        for b in range(1, n):
            count = count + tk[b]
        return 1.0 / count[0:1, 0:1]

    def finish_value(scale):
        for h in range(2):
            dw1[h] = dot(xg[h], gq[t], 0, 0) * scale

    def finish_output(scale):
        for h in range(2):
            dw2[h] = dot(pj[t], us[h], 0, 0) * scale

    def drain_common():
        sent("w", 0, w1o)
        sent("w", 1, w2o)

        def one(b):
            sent("tk", b, tk.at[b])
            sent("p", b, pb.at[blk(b)])
            sent("q", b, qb.at[blk(b)])
            sent("pj", b, pj.at[t, blk(b)])
            sent("gq", b, gq.at[t, blk(b)])
        others(one)

    def first_section():
        start_common()
        all_to_all(xs)
        forward_chunk(j, False)

        def chunk(b):
            arrive("a", "xf", xs, b)
            forward_chunk(b, False)
        others(chunk)
        forward_out()

        def back(b):
            arrive("g", "uf", us, b)
            backward_chunk(b)
        everyone(back)
        scale = tokens()
        reduce("q", qb, qr, qacc)
        gq[t, blk(j)] = (rkeep[:, :1] * qacc[...]).astype(BF)
        share("gq", gq, False)
        finish_output(scale)
        others(lambda b: got("gq", b, gq.at[t, blk(b)]))
        finish_value(scale)
        got("w", 0, w1o)
        drain_common()

        def rest(b):
            sent("a", b, src.at[0])
            sent("xf", b, xs.at[t, blk(b)])
        others(rest)

        def rest_all(b):
            sent("pjf", b, pj.at[t, blk(b)])
            sent("x", b, yx.at[blk(b)])
            sent("uf", b, us.at[t, blk(b)])
        everyone(rest_all)

    def middle_section():
        start_common()

        def chunk(b):
            arrive("x", "xf", xs, b)
            forward_chunk(b, False)
        everyone(chunk)
        forward_out()

        def back(b):
            arrive("g", "uf", us, b)
            backward_chunk(b)
        everyone(back)
        backward_out(False)
        scale = tokens()
        finish_output(scale)
        finish_value(scale)
        drain_common()
        sent("e", 0, exs)
        others(lambda b: sent("sc", b, sc.at[b]))

        def rest_all(b):
            sent("xf", b, xs.at[t, blk(b)])
            sent("uf", b, us.at[t, blk(b)])
            sent("pjf", b, pj.at[t, blk(b)])
            sent("gqf", b, gq.at[t, blk(b)])
            sent("x", b, yx.at[blk(b)])
            sent("g", b, yg.at[blk(b)])
        everyone(rest_all)

    def last_section():
        start_common()
        all_to_all(us)
        backward_chunk(j)

        def seeds(b):
            arrive("a", "uf", us, b)
            backward_chunk(b)
        others(seeds)

        def chunk(b):
            arrive("x", "xf", xs, b)
            forward_chunk(b, True)
        everyone(chunk)
        reduce("p", pb, pr, pacc)
        own_inverse()
        backward_out(True)
        scale = tokens()
        finish_value(scale)
        others(lambda b: got("pj", b, pj.at[t, blk(b)]))
        finish_output(scale)
        got("w", 1, w2o)
        drain_common()
        sent("e", 0, exs)

        def rest(b):
            sent("a", b, src.at[0])
            sent("uf", b, us.at[t, blk(b)])
            sent("sc", b, sc.at[b])
        others(rest)

        def rest_all(b):
            sent("xf", b, xs.at[t, blk(b)])
            sent("gqf", b, gq.at[t, blk(b)])
            sent("g", b, yg.at[blk(b)])
        everyone(rest_all)

    pl.when(s == 0)(first_section)
    pl.when(s == last)(last_section)
    if sections > 2:
        pl.when((s > 0) & (s < last))(middle_section)


def local(
    hidden, unembed, value_proj, output_proj, norm_gains, survive, lengths, assign,
    advantage, reference_logit, recorded_gap,
):
    n = lax.axis_size("dp")
    sections = lax.axis_size("section")
    j = lax.axis_index("dp")
    s = lax.axis_index("section")
    count, positions, width = hidden.shape
    rows = count * positions
    part = value_proj.shape[1]
    half = part // 2
    v = value_proj.shape[2]
    group = count // survive.shape[0]

    src = jnp.where(s == sections - 1, unembed, hidden).reshape(rows, n * 2, half)
    src = src.transpose(1, 0, 2)
    w1 = value_proj[0].reshape(2, half, v)
    w2 = output_proj[0].reshape(v, 2, half).transpose(1, 0, 2)
    gain = lax.dynamic_slice(norm_gains[0], (j * part,), (part,)).reshape(2, 1, half)
    present = jnp.sum(
        (assign[None, :] == jnp.arange(count, dtype=jnp.int32)[:, None]).astype(F32), axis=1
    )
    live = (
        lax.broadcasted_iota(jnp.int32, (count, positions), 1) < lengths[:, None]
    ).astype(F32)
    adv = advantage[:, None]
    clipped = ((adv > 0) & (recorded_gap > clip_high)) | ((adv < 0) & (recorded_gap < clip_low))
    weight = -loss_scale * adv * (1.0 - clipped.astype(F32)) * live * present[:, None]
    rinfo = jnp.stack([weight.reshape(rows), reference_logit.reshape(rows)], axis=1)
    tok = jnp.sum((jnp.repeat(survive, group) * lengths).astype(F32))
    tok = jnp.broadcast_to(tok, (8, LANES))

    total = n * rows
    kinds = len(KINDS)
    vm = pl.BlockSpec(memory_space=pltpu.VMEM)
    dw1, dw2 = pl.pallas_call(
        functools.partial(kernel, n, sections, width),
        out_shape=(
            jax.ShapeDtypeStruct((2, half, v), F32),
            jax.ShapeDtypeStruct((2, v, half), F32),
        ),
        in_specs=[vm] * 6,
        out_specs=(vm, vm),
        scratch_shapes=[
            pltpu.VMEM((2, total, half), BF),
            pltpu.VMEM((2, total, half), BF),
            pltpu.VMEM((2, total, half), BF),
            pltpu.VMEM((total, v + LANES), BF),
            pltpu.VMEM((n, rows, v + LANES), BF),
            pltpu.VMEM((total, v), BF),
            pltpu.VMEM((n, rows, v), BF),
            pltpu.VMEM((2, total, v), BF),
            pltpu.VMEM((2, total, v), BF),
            pltpu.VMEM((n, rows, LANES), BF),
            pltpu.VMEM((half, v), BF),
            pltpu.VMEM((v, half), BF),
            pltpu.VMEM((total, half), BF),
            pltpu.VMEM((total, half), BF),
            pltpu.VMEM((n, 8, LANES), F32),
            pltpu.VMEM((rows, LANES), F32),
            pltpu.VMEM((rows, LANES), F32),
            pltpu.VMEM((rows, v + LANES), F32),
            pltpu.VMEM((rows, v), F32),
            pltpu.VMEM((rows, LANES), F32),
            pltpu.SemaphoreType.DMA((kinds, n)),
            pltpu.SemaphoreType.DMA((kinds, n)),
        ],
        compiler_params=pltpu.CompilerParams(
            collective_id=0, has_side_effects=True, vmem_limit_bytes=60 * 1024 * 1024
        ),
    )(src, w1, w2, gain, rinfo, tok)
    return (
        dw1.reshape(1, part, v),
        dw2.transpose(1, 0, 2).reshape(1, v, part),
    )


def solution(mesh):
    rowwise = P(("groups", "dp"))
    placed = (
        P(("groups", "dp"), None, None),
        P(("groups", "dp"), None, None),
        P("section", "dp", "tensor"),
        P("section", "tensor", "dp"),
        P("section", None),
        rowwise,
        rowwise,
        rowwise,
        rowwise,
        P(("groups", "dp"), None),
        P(("groups", "dp"), None),
    )
    return jax.shard_map(
        local,
        mesh=mesh,
        in_specs=placed,
        out_specs=(
            P(("groups", "section"), "dp", "tensor"),
            P(("groups", "section"), "tensor", "dp"),
        ),
        check_vma=False,
    )
```

```python
import functools
import math

import jax
import jax.numpy as jnp
from jax import lax
from jax.experimental import pallas as pl
from jax.experimental.pallas import tpu as pltpu
from jax.sharding import PartitionSpec as P

eps_norm = 1e-06
loss_scale = 4096.0
clip_high = math.log(1.28)
clip_low = math.log(0.8)
LANES = 128
KINDS = ("a", "xf", "uf", "p", "q", "pj", "pjf", "gq", "gqf", "sc", "tk", "x", "g", "w", "e", "ps")
BF = jnp.bfloat16
F32 = jnp.float32


def dot(a, b, ca=1, cb=0):
    return lax.dot_general(a, b, (((ca,), (cb,)), ((), ())), preferred_element_type=F32)


def kernel(
    n, sections, width,
    src, w1, w2, gains, survive, lengths, assign, advantage, base, gap,
    dw1, dw2,
    xs, us, xg, pb, pr, qb, qr, pj, gq, sc, w1o, w2o, yx, yg, tk, exs, exr, pacc, qacc, rkeep,
    ps, psr, rinfo, tok,
    ss, rs,
):
    j = lax.axis_index("dp")
    s = lax.axis_index("section")
    t = lax.axis_index("tensor")
    o = 1 - t
    rows = src.shape[1]
    v = w1.shape[2]
    last = sections - 1
    partner = {"tensor": o}
    count, positions = base.shape

    def gain(h):
        return gains[j * 2 + h]

    def own_tokens():
        response = lax.broadcasted_iota(jnp.int32, (1, count), 1)
        group = count // survive.shape[1]
        kept = jnp.zeros((1, count), F32)
        for g in range(survive.shape[1]):
            inside = (response >= g * group) & (response < (g + 1) * group)
            kept = jnp.where(inside, survive[0:1, g:g + 1].astype(F32), kept)
        held = jnp.sum(kept * lengths[...].astype(F32), axis=1, keepdims=True)
        tok[...] = jnp.broadcast_to(held, (8, LANES))

    def row_info():
        row = lax.broadcasted_iota(jnp.int32, (rows, count), 0)
        first = lax.broadcasted_iota(jnp.int32, (rows, count), 1) * positions
        mine = (row >= first) & (row < first + positions)
        diagonal = lax.broadcasted_iota(jnp.int32, (count, positions, positions), 1)
        diagonal = diagonal == lax.broadcasted_iota(
            jnp.int32, (count, positions, positions), 2
        )

        def by_response(values):
            return jnp.sum(jnp.where(mine, values, 0.0), axis=1, keepdims=True)

        def by_position(values):
            spread = jnp.where(diagonal, values[:, None, :], 0.0)
            return jnp.sum(spread, axis=2, keepdims=True).reshape(rows, 1)

        slots = assign[...]
        starts = slots * positions
        hit = (row >= starts) & (row < starts + positions)
        listed = jnp.sum(jnp.where(hit, 1.0, 0.0), axis=1, keepdims=True)
        start = by_response(first.astype(F32))
        place = lax.broadcasted_iota(jnp.int32, (rows, 1), 0).astype(F32) - start
        live = place < by_response(lengths[...].astype(F32))
        adv = by_response(advantage[...])
        q = by_position(gap[...])
        clipped = ((adv > 0) & (q > clip_high)) | ((adv < 0) & (q < clip_low))
        weight = jnp.where(clipped | (~live), 0.0, -loss_scale * adv * listed)
        rinfo[...] = jnp.where(lane == 0, weight, jnp.where(lane == 1, by_position(base[...]), 0.0))

    def blk(b):
        return pl.ds(pl.multiple_of(b * rows, rows), rows)

    def peer(k):
        return lax.rem(j + k, n)

    def send(kind, si, ri, a, b, dev):
        k = KINDS.index(kind)
        pltpu.make_async_remote_copy(
            src_ref=a, dst_ref=b, send_sem=ss.at[k, si], recv_sem=rs.at[k, ri],
            device_id=dev, device_id_type=pl.DeviceIdType.MESH,
        ).start()

    def handle(kind, i, a):
        k = KINDS.index(kind)
        return pltpu.make_async_remote_copy(
            src_ref=a, dst_ref=a, send_sem=ss.at[k, i], recv_sem=rs.at[k, i],
            device_id=partner, device_id_type=pl.DeviceIdType.MESH,
        )

    def got(kind, i, a):
        handle(kind, i, a).wait_recv()

    def sent(kind, i, a):
        handle(kind, i, a).wait_send()

    def others(body):
        def step(k, carry):
            body(peer(k))
            return carry
        lax.fori_loop(1, n, step, 0)

    def everyone(body):
        def step(k, carry):
            body(peer(k))
            return carry
        lax.fori_loop(0, n, step, 0)

    barrier = pltpu.get_barrier_semaphore()

    def greet(dev):
        pl.semaphore_signal(barrier, inc=1, device_id=dev, device_id_type=pl.DeviceIdType.MESH)

    for k in range(1, n):
        greet({"dp": peer(k)})
    greet(partner)

    @pl.when(s > 0)
    def _():
        greet({"section": s - 1})

    @pl.when(s < last)
    def _():
        greet({"section": s + 1})

    pl.semaphore_wait(barrier, n + jnp.where(s > 0, 1, 0) + jnp.where(s < last, 1, 0))

    def start_common():
        send("w", 0, 0, w1.at[o], w1o, partner)
        send("w", 1, 1, w2.at[o], w2o, partner)
        own_tokens()
        others(lambda b: send("tk", b, j, tok, tk.at[j], {"dp": b}))
        tk[j] = tok[...]

    def all_to_all(dst):
        others(lambda b: send("a", b, j, src.at[b * 2 + t], dst.at[t, blk(j)], {"dp": b}))
        dst[0, blk(j)] = src[j * 2]
        dst[1, blk(j)] = src[j * 2 + 1]

    def arrive(kind, fkind, buf, b):
        got(kind, b, buf.at[t, blk(b)])
        send(fkind, b, b, buf.at[t, blk(b)], buf.at[t, blk(b)], partner)
        got(fkind, b, buf.at[o, blk(b)])

    lane = lax.broadcasted_iota(jnp.int32, (rows, LANES), 1)

    def pack(values):
        packed = jnp.zeros((rows, LANES), F32)
        for i, value in enumerate(values):
            packed = jnp.where(lane == i, value, packed)
        return packed.T[:8]

    def unpack(packed):
        filled = jnp.concatenate([packed, jnp.zeros((LANES - 8, rows), F32)], axis=0)
        return filled.T

    def forward_chunk(b, with_logit):
        total = jnp.zeros((rows, v), F32)
        squares = jnp.zeros((rows, 1), F32)
        logit = jnp.zeros((rows, 1), F32)
        for h in range(2):
            x = xs[h, blk(b)].astype(F32)
            squares += jnp.sum(x * x, axis=1, keepdims=True)
            if with_logit:
                logit += jnp.sum(x * us[h, blk(b)].astype(F32), axis=1, keepdims=True)
            scaled = (x * gain(h)).astype(BF)
            xg[h, blk(b)] = scaled
            total += dot(scaled, w1[h])
        pb[blk(b)] = total.astype(BF)
        ps[b] = pack([squares, logit] if with_logit else [squares])

        @pl.when(b != j)
        def _():
            send("p", b, j, pb.at[blk(b)], pr.at[j], {"dp": b})
            send("ps", b, j, ps.at[b], psr.at[j], {"dp": b})

    def backward_chunk(b):
        total = dot(us[0, blk(b)], w2[0], 1, 1) + dot(us[1, blk(b)], w2[1], 1, 1)
        qb[blk(b)] = total.astype(BF)

        @pl.when(b != j)
        def _():
            send("q", b, j, qb.at[blk(b)], qr.at[j], {"dp": b})

    def reduce(kind, own, landed, acc):
        acc[...] = own[blk(j)].astype(F32)

        def add(b):
            got(kind, b, landed.at[b])
            acc[...] += landed[b].astype(F32)
        others(add)

    def share(kind, buf, forward):
        others(lambda b: send(kind, b, j, buf.at[t, blk(j)], buf.at[t, blk(j)], {"dp": b}))
        if forward:
            send(kind + "f", j, j, buf.at[t, blk(j)], buf.at[t, blk(j)], partner)

    def shared(kind, buf, b):
        @pl.when(b != j)
        def _():
            got(kind, b, buf.at[t, blk(b)])
            send(kind + "f", b, b, buf.at[t, blk(b)], buf.at[t, blk(b)], partner)
        got(kind + "f", b, buf.at[o, blk(b)])

    def own_inverse():
        psr[j] = ps[j]
        others(lambda b: got("ps", b, psr.at[b]))
        sums = psr[0]
        for b in range(1, n):
            sums = sums + psr[b]
        sums = unpack(sums)
        inverse = lax.rsqrt(sums[:, 0:1] / width + eps_norm)
        rkeep[...] = jnp.where(lane == 0, inverse, sums)
        return inverse

    def forward_out():
        inverse = own_inverse()
        reduce("p", pb, pr, pacc)
        pj[t, blk(j)] = (inverse * pacc[...]).astype(BF)
        share("pj", pj, True)
        got("w", 1, w2o)

        def chunk(b):
            shared("pj", pj, b)
            mixed = dot(pj[t, blk(b)], w2[t]) + dot(pj[o, blk(b)], w2o[...])
            yx[blk(b)] = (xs[t, blk(b)].astype(F32) + mixed).astype(BF)
            send("x", b, b, yx.at[blk(b)], xs.at[t, blk(b)], {"section": s + 1})
        everyone(chunk)

    def dot_over_units():
        exs[...] = jnp.broadcast_to(
            jnp.sum(pacc[...] * qacc[...], axis=1, keepdims=True), (rows, LANES)
        )
        send("e", 0, 0, exs, exr, partner)
        got("e", 0, exr)
        return exs[:, :1] + exr[:, :1]

    def backward_out(is_last):
        reduce("q", qb, qr, qacc)
        inner = dot_over_units()
        inverse = rkeep[:, :1]
        if is_last:
            logit = rkeep[:, 1:2] + inverse * inner
            seed = rinfo[:, 0:1] * jnp.exp(logit - rinfo[:, 1:2])
            scale = seed * inverse
            pj[t, blk(j)] = (scale * pacc[...]).astype(BF)
        else:
            seed = jnp.ones((rows, 1), F32)
            scale = inverse
        gq[t, blk(j)] = (scale * qacc[...]).astype(BF)
        sc[j] = pack([inverse * inverse * inverse * (seed * inner) / width, seed])
        share("gq", gq, True)
        others(lambda b: send("sc", b, j, sc.at[j], sc.at[j], {"dp": b}))
        got("w", 0, w1o)

        def chunk(b):
            shared("gq", gq, b)

            @pl.when(b != j)
            def _():
                got("sc", b, sc.at[b])
            packed = unpack(sc[b])
            grad = dot(gq[t, blk(b)], w1[t], 1, 1) + dot(gq[o, blk(b)], w1o[...], 1, 1)
            upstream = us[t, blk(b)].astype(F32)
            if is_last:
                upstream = packed[:, 1:2] * upstream
            yg[blk(b)] = (
                upstream + gain(t) * grad - packed[:, 0:1] * xs[t, blk(b)].astype(F32)
            ).astype(BF)
            send("g", b, b, yg.at[blk(b)], us.at[t, blk(b)], {"section": s - 1})
        everyone(chunk)

    def tokens():
        others(lambda b: got("tk", b, tk.at[b]))
        count = tk[0]
        for b in range(1, n):
            count = count + tk[b]
        return 1.0 / count[0:1, 0:1]

    def finish_value(scale):
        for h in range(2):
            dw1[h] = dot(xg[h], gq[t], 0, 0) * scale

    def finish_value_arriving(scale):
        def add(b, start):
            for h in range(2):
                part = dot(xg[h, blk(b)], gq[t, blk(b)], 0, 0) * scale
                dw1[h] = part if start else dw1[h] + part
        add(j, True)

        def later(b):
            got("gq", b, gq.at[t, blk(b)])
            add(b, False)
        others(later)

    def finish_output(scale):
        for h in range(2):
            dw2[h] = dot(pj[t], us[h], 0, 0) * scale

    def drain_common():
        sent("w", 0, w1o)
        sent("w", 1, w2o)

        def one(b):
            sent("tk", b, tk.at[b])
            sent("p", b, pb.at[blk(b)])
            sent("ps", b, ps.at[b])
            sent("q", b, qb.at[blk(b)])
            sent("pj", b, pj.at[t, blk(b)])
            sent("gq", b, gq.at[t, blk(b)])
        others(one)

    def first_section():
        start_common()
        all_to_all(xs)
        forward_chunk(j, False)

        def chunk(b):
            arrive("a", "xf", xs, b)
            forward_chunk(b, False)
        others(chunk)
        forward_out()

        def back(b):
            arrive("g", "uf", us, b)
            backward_chunk(b)
        everyone(back)
        scale = tokens()
        reduce("q", qb, qr, qacc)
        gq[t, blk(j)] = (rkeep[:, :1] * qacc[...]).astype(BF)
        share("gq", gq, False)
        finish_output(scale)
        finish_value_arriving(scale)
        got("w", 0, w1o)
        drain_common()

        def rest(b):
            sent("a", b, src.at[0])
            sent("xf", b, xs.at[t, blk(b)])
        others(rest)

        def rest_all(b):
            sent("pjf", b, pj.at[t, blk(b)])
            sent("x", b, yx.at[blk(b)])
            sent("uf", b, us.at[t, blk(b)])
        everyone(rest_all)

    def middle_section():
        start_common()

        def chunk(b):
            arrive("x", "xf", xs, b)
            forward_chunk(b, False)
        everyone(chunk)
        forward_out()

        def back(b):
            arrive("g", "uf", us, b)
            backward_chunk(b)
        everyone(back)
        backward_out(False)
        scale = tokens()
        finish_output(scale)
        finish_value(scale)
        drain_common()
        sent("e", 0, exs)
        others(lambda b: sent("sc", b, sc.at[b]))

        def rest_all(b):
            sent("xf", b, xs.at[t, blk(b)])
            sent("uf", b, us.at[t, blk(b)])
            sent("pjf", b, pj.at[t, blk(b)])
            sent("gqf", b, gq.at[t, blk(b)])
            sent("x", b, yx.at[blk(b)])
            sent("g", b, yg.at[blk(b)])
        everyone(rest_all)

    def last_section():
        start_common()
        all_to_all(us)
        backward_chunk(j)
        row_info()

        def seeds(b):
            arrive("a", "uf", us, b)
            backward_chunk(b)
        others(seeds)

        def chunk(b):
            arrive("x", "xf", xs, b)
            forward_chunk(b, True)
        everyone(chunk)
        own_inverse()
        reduce("p", pb, pr, pacc)
        backward_out(True)
        share("pj", pj, False)
        scale = tokens()
        finish_value(scale)
        others(lambda b: got("pj", b, pj.at[t, blk(b)]))
        finish_output(scale)
        got("w", 1, w2o)
        drain_common()
        sent("e", 0, exs)

        def rest(b):
            sent("a", b, src.at[0])
            sent("uf", b, us.at[t, blk(b)])
            sent("sc", b, sc.at[b])
        others(rest)

        def rest_all(b):
            sent("xf", b, xs.at[t, blk(b)])
            sent("gqf", b, gq.at[t, blk(b)])
            sent("g", b, yg.at[blk(b)])
        everyone(rest_all)

    pl.when(s == 0)(first_section)
    pl.when(s == last)(last_section)
    if sections > 2:
        pl.when((s > 0) & (s < last))(middle_section)


def local(
    hidden, unembed, value_proj, output_proj, norm_gains, survive, lengths, assign,
    advantage, reference_logit, recorded_gap,
):
    n = lax.axis_size("dp")
    sections = lax.axis_size("section")
    s = lax.axis_index("section")
    count, positions, width = hidden.shape
    rows = count * positions
    part = value_proj.shape[1]
    half = part // 2
    v = value_proj.shape[2]

    src = jnp.where(s == sections - 1, unembed, hidden).reshape(rows, n * 2, half)
    src = src.transpose(1, 0, 2)
    w1 = value_proj[0].reshape(2, half, v)
    w2 = output_proj[0].reshape(v, 2, half).transpose(1, 0, 2)
    gains = norm_gains[0].reshape(n * 2, 1, half)
    total = n * rows
    kinds = len(KINDS)
    vm = pl.BlockSpec(memory_space=pltpu.VMEM)
    dw1, dw2 = pl.pallas_call(
        functools.partial(kernel, n, sections, width),
        out_shape=(
            jax.ShapeDtypeStruct((2, half, v), F32),
            jax.ShapeDtypeStruct((2, v, half), F32),
        ),
        in_specs=[vm] * 10,
        out_specs=(vm, vm),
        scratch_shapes=[
            pltpu.VMEM((2, total, half), BF),
            pltpu.VMEM((2, total, half), BF),
            pltpu.VMEM((2, total, half), BF),
            pltpu.VMEM((total, v), BF),
            pltpu.VMEM((n, rows, v), BF),
            pltpu.VMEM((total, v), BF),
            pltpu.VMEM((n, rows, v), BF),
            pltpu.VMEM((2, total, v), BF),
            pltpu.VMEM((2, total, v), BF),
            pltpu.VMEM((n, 8, rows), F32),
            pltpu.VMEM((half, v), BF),
            pltpu.VMEM((v, half), BF),
            pltpu.VMEM((total, half), BF),
            pltpu.VMEM((total, half), BF),
            pltpu.VMEM((n, 8, LANES), F32),
            pltpu.VMEM((rows, LANES), F32),
            pltpu.VMEM((rows, LANES), F32),
            pltpu.VMEM((rows, v), F32),
            pltpu.VMEM((rows, v), F32),
            pltpu.VMEM((rows, LANES), F32),
            pltpu.VMEM((n, 8, rows), F32),
            pltpu.VMEM((n, 8, rows), F32),
            pltpu.VMEM((rows, LANES), F32),
            pltpu.VMEM((8, LANES), F32),
            pltpu.SemaphoreType.DMA((kinds, n)),
            pltpu.SemaphoreType.DMA((kinds, n)),
        ],
        compiler_params=pltpu.CompilerParams(
            collective_id=0, has_side_effects=True, vmem_limit_bytes=60 * 1024 * 1024
        ),
    )(
        src, w1, w2, gains, survive.reshape(1, -1), lengths.reshape(1, count),
        assign.reshape(1, count), advantage.reshape(1, count), reference_logit, recorded_gap,
    )
    return (
        dw1.reshape(1, part, v),
        dw2.transpose(1, 0, 2).reshape(1, v, part),
    )


def solution(mesh):
    rowwise = P(("groups", "dp"))
    placed = (
        P(("groups", "dp"), None, None),
        P(("groups", "dp"), None, None),
        P("section", "dp", "tensor"),
        P("section", "tensor", "dp"),
        P("section", None),
        rowwise,
        rowwise,
        rowwise,
        rowwise,
        P(("groups", "dp"), None),
        P(("groups", "dp"), None),
    )
    return jax.shard_map(
        local,
        mesh=mesh,
        in_specs=placed,
        out_specs=(
            P(("groups", "section"), "dp", "tensor"),
            P(("groups", "section"), "tensor", "dp"),
        ),
        check_vma=False,
    )
```

```python
import functools
import math

import jax
import jax.numpy as jnp
from jax import lax
from jax.experimental import pallas as pl
from jax.experimental.pallas import tpu as pltpu
from jax.sharding import PartitionSpec as P

eps_norm = 1e-06
loss_scale = 4096.0
clip_high = math.log(1.28)
clip_low = math.log(0.8)
LANES = 128
KINDS = ("a", "xf", "uf", "p", "q", "pj", "pjf", "gq", "gqf", "sc", "tk", "x", "g", "w", "e", "ps")
BF = jnp.bfloat16
F32 = jnp.float32


def dot(a, b, ca=1, cb=0):
    return lax.dot_general(a, b, (((ca,), (cb,)), ((), ())), preferred_element_type=F32)


def kernel(
    n, sections, width,
    src, w1, w2, gains, survive, lengths, assign, advantage, base, gap,
    dw1, dw2,
    xs, us, xg, pb, pr, qb, qr, pj, gq, sc, w1o, w2o, yx, yg, tk, exs, exr, pacc, qacc, rkeep,
    ps, psr, rinfo, tok,
    ss, rs,
):
    j = lax.axis_index("dp")
    s = lax.axis_index("section")
    t = lax.axis_index("tensor")
    o = 1 - t
    rows = src.shape[1]
    half, v = w1.shape[1:]
    last = sections - 1
    partner = {"tensor": o}
    positions, count = base.shape

    def gain(h):
        return gains[j * 2 + h]

    def own_tokens():
        response = lax.broadcasted_iota(jnp.int32, (1, count), 1)
        group = count // survive.shape[1]
        kept = jnp.zeros((1, count), F32)
        for g in range(survive.shape[1]):
            inside = (response >= g * group) & (response < (g + 1) * group)
            kept = jnp.where(inside, survive[0:1, g:g + 1].astype(F32), kept)
        held = jnp.sum(kept * lengths[...].astype(F32), axis=1, keepdims=True)
        tok[...] = jnp.broadcast_to(held, (8, LANES))

    def row_info():
        row = lax.broadcasted_iota(jnp.int32, (rows, count), 0)
        first = lax.broadcasted_iota(jnp.int32, (rows, count), 1) * positions
        mine = (row >= first) & (row < first + positions)

        def by_response(values):
            return jnp.sum(jnp.where(mine, values, 0.0), axis=1, keepdims=True)

        def by_position(values):
            return by_response(jnp.concatenate([values] * count, axis=0))

        slots = assign[...]
        starts = slots * positions
        hit = (row >= starts) & (row < starts + positions)
        listed = jnp.sum(jnp.where(hit, 1.0, 0.0), axis=1, keepdims=True)
        start = by_response(first.astype(F32))
        place = lax.broadcasted_iota(jnp.int32, (rows, 1), 0).astype(F32) - start
        live = place < by_response(lengths[...].astype(F32))
        adv = by_response(advantage[...])
        q = by_position(gap[...])
        clipped = ((adv > 0) & (q > clip_high)) | ((adv < 0) & (q < clip_low))
        weight = jnp.where(clipped | (~live), 0.0, -loss_scale * adv * listed)
        rinfo[...] = jnp.where(lane == 0, weight, jnp.where(lane == 1, by_position(base[...]), 0.0))

    def blk(b):
        return pl.ds(pl.multiple_of(b * rows, rows), rows)

    def peer(k):
        return lax.rem(j + k, n)

    def send(kind, si, ri, a, b, dev):
        k = KINDS.index(kind)
        pltpu.make_async_remote_copy(
            src_ref=a, dst_ref=b, send_sem=ss.at[k, si], recv_sem=rs.at[k, ri],
            device_id=dev, device_id_type=pl.DeviceIdType.MESH,
        ).start()

    def handle(kind, i, a):
        k = KINDS.index(kind)
        return pltpu.make_async_remote_copy(
            src_ref=a, dst_ref=a, send_sem=ss.at[k, i], recv_sem=rs.at[k, i],
            device_id=partner, device_id_type=pl.DeviceIdType.MESH,
        )

    def got(kind, i, a):
        handle(kind, i, a).wait_recv()

    def sent(kind, i, a):
        handle(kind, i, a).wait_send()

    def others(body):
        def step(k, carry):
            body(peer(k))
            return carry
        lax.fori_loop(1, n, step, 0)

    def everyone(body):
        def step(k, carry):
            body(peer(k))
            return carry
        lax.fori_loop(0, n, step, 0)

    barrier = pltpu.get_barrier_semaphore()

    def greet(dev):
        pl.semaphore_signal(barrier, inc=1, device_id=dev, device_id_type=pl.DeviceIdType.MESH)

    for k in range(1, n):
        greet({"dp": peer(k)})
    greet(partner)

    @pl.when(s > 0)
    def _():
        greet({"section": s - 1})

    @pl.when(s < last)
    def _():
        greet({"section": s + 1})

    pl.semaphore_wait(barrier, n + jnp.where(s > 0, 1, 0) + jnp.where(s < last, 1, 0))

    def start_common():
        send("w", 0, 0, w1.at[o], w1o, partner)
        send("w", 1, 1, w2.at[o], w2o, partner)
        own_tokens()
        others(lambda b: send("tk", b, j, tok, tk.at[j], {"dp": b}))
        tk[j] = tok[...]

    def all_to_all(dst):
        others(lambda b: send("a", b, j, src.at[b * 2 + t], dst.at[t, blk(j)], {"dp": b}))
        dst[0, blk(j)] = src[j * 2]
        dst[1, blk(j)] = src[j * 2 + 1]

    def arrive(kind, fkind, buf, b):
        got(kind, b, buf.at[t, blk(b)])
        send(fkind, b, b, buf.at[t, blk(b)], buf.at[t, blk(b)], partner)
        got(fkind, b, buf.at[o, blk(b)])

    lane = lax.broadcasted_iota(jnp.int32, (rows, LANES), 1)

    def pack(values):
        packed = jnp.zeros((rows, LANES), F32)
        for i, value in enumerate(values):
            packed = jnp.where(lane == i, value, packed)
        return packed.T[:8]

    def unpack(packed):
        filled = jnp.concatenate([packed, jnp.zeros((LANES - 8, rows), F32)], axis=0)
        return filled.T

    def forward_chunk(b, with_logit):
        total = jnp.zeros((rows, v), F32)
        squares = jnp.zeros((rows, 1), F32)
        logit = jnp.zeros((rows, 1), F32)
        for h in range(2):
            x = xs[h, blk(b)].astype(F32)
            squares += jnp.sum(x * x, axis=1, keepdims=True)
            if with_logit:
                logit += jnp.sum(x * us[h, blk(b)].astype(F32), axis=1, keepdims=True)
            scaled = (x * gain(h)).astype(BF)
            xg[h, blk(b)] = scaled
            total += dot(scaled, w1[h])
        pb[blk(b)] = total.astype(BF)
        ps[b] = pack([squares, logit] if with_logit else [squares])

        @pl.when(b != j)
        def _():
            send("p", b, j, pb.at[blk(b)], pr.at[j], {"dp": b})
            send("ps", b, j, ps.at[b], psr.at[j], {"dp": b})

    def backward_chunk(b):
        total = dot(us[0, blk(b)], w2[0], 1, 1) + dot(us[1, blk(b)], w2[1], 1, 1)
        qb[blk(b)] = total.astype(BF)

        @pl.when(b != j)
        def _():
            send("q", b, j, qb.at[blk(b)], qr.at[j], {"dp": b})

    def reduce(kind, own, landed, acc):
        acc[...] = own[blk(j)].astype(F32)

        def add(b):
            got(kind, b, landed.at[b])
            acc[...] += landed[b].astype(F32)
        others(add)

    def share(kind, buf, forward):
        others(lambda b: send(kind, b, j, buf.at[t, blk(j)], buf.at[t, blk(j)], {"dp": b}))
        if forward:
            send(kind + "f", j, j, buf.at[t, blk(j)], buf.at[t, blk(j)], partner)

    def shared(kind, buf, b):
        @pl.when(b != j)
        def _():
            got(kind, b, buf.at[t, blk(b)])
            send(kind + "f", b, b, buf.at[t, blk(b)], buf.at[t, blk(b)], partner)
        got(kind + "f", b, buf.at[o, blk(b)])

    def own_inverse():
        psr[j] = ps[j]
        others(lambda b: got("ps", b, psr.at[b]))
        sums = psr[0]
        for b in range(1, n):
            sums = sums + psr[b]
        sums = unpack(sums)
        inverse = lax.rsqrt(sums[:, 0:1] / width + eps_norm)
        rkeep[...] = jnp.where(lane == 0, inverse, sums)
        return inverse

    def forward_out():
        inverse = own_inverse()
        reduce("p", pb, pr, pacc)
        pj[t, blk(j)] = (inverse * pacc[...]).astype(BF)
        share("pj", pj, True)
        got("w", 1, w2o)

        def chunk(b):
            shared("pj", pj, b)
            mixed = dot(pj[t, blk(b)], w2[t]) + dot(pj[o, blk(b)], w2o[...])
            yx[blk(b)] = (xs[t, blk(b)].astype(F32) + mixed).astype(BF)
            send("x", b, b, yx.at[blk(b)], xs.at[t, blk(b)], {"section": s + 1})
        everyone(chunk)

    def dot_over_units():
        exs[...] = jnp.broadcast_to(
            jnp.sum(pacc[...] * qacc[...], axis=1, keepdims=True), (rows, LANES)
        )
        send("e", 0, 0, exs, exr, partner)
        got("e", 0, exr)
        return exs[:, :1] + exr[:, :1]

    def backward_out(is_last):
        reduce("q", qb, qr, qacc)
        inner = dot_over_units()
        inverse = rkeep[:, :1]
        if is_last:
            logit = rkeep[:, 1:2] + inverse * inner
            seed = rinfo[:, 0:1] * jnp.exp(logit - rinfo[:, 1:2])
            scale = seed * inverse
            pj[t, blk(j)] = (scale * pacc[...]).astype(BF)
        else:
            seed = jnp.ones((rows, 1), F32)
            scale = inverse
        gq[t, blk(j)] = (scale * qacc[...]).astype(BF)
        sc[j] = pack([inverse * inverse * inverse * (seed * inner) / width, seed])
        share("gq", gq, True)
        others(lambda b: send("sc", b, j, sc.at[j], sc.at[j], {"dp": b}))
        got("w", 0, w1o)

        def chunk(b):
            shared("gq", gq, b)

            @pl.when(b != j)
            def _():
                got("sc", b, sc.at[b])
            packed = unpack(sc[b])
            grad = dot(gq[t, blk(b)], w1[t], 1, 1) + dot(gq[o, blk(b)], w1o[...], 1, 1)
            upstream = us[t, blk(b)].astype(F32)
            if is_last:
                upstream = packed[:, 1:2] * upstream
            yg[blk(b)] = (
                upstream + gain(t) * grad - packed[:, 0:1] * xs[t, blk(b)].astype(F32)
            ).astype(BF)
            send("g", b, b, yg.at[blk(b)], us.at[t, blk(b)], {"section": s - 1})
        everyone(chunk)

    def tokens():
        others(lambda b: got("tk", b, tk.at[b]))
        count = tk[0]
        for b in range(1, n):
            count = count + tk[b]
        return 1.0 / count[0:1, 0:1]

    def finish_value(scale):
        for h in range(2):
            dw1[h] = dot(xg[h], gq[t], 0, 0) * scale

    def finish_value_arriving(scale):
        def add(b, start):
            for h in range(2):
                part = dot(xg[h, blk(b)], gq[t, blk(b)], 0, 0) * scale
                dw1[h] = part if start else dw1[h] + part
        add(j, True)

        def later(b):
            got("gq", b, gq.at[t, blk(b)])
            add(b, False)
        others(later)

    def finish_output(scale):
        for h in range(2):
            dw2[:, h * half:(h + 1) * half] = dot(pj[t], us[h], 0, 0) * scale

    def drain_common():
        sent("w", 0, w1o)
        sent("w", 1, w2o)

        def one(b):
            sent("tk", b, tk.at[b])
            sent("p", b, pb.at[blk(b)])
            sent("ps", b, ps.at[b])
            sent("q", b, qb.at[blk(b)])
            sent("pj", b, pj.at[t, blk(b)])
            sent("gq", b, gq.at[t, blk(b)])
        others(one)

    def first_section():
        start_common()
        all_to_all(xs)
        forward_chunk(j, False)

        def chunk(b):
            arrive("a", "xf", xs, b)
            forward_chunk(b, False)
        others(chunk)
        forward_out()

        def back(b):
            arrive("g", "uf", us, b)
            backward_chunk(b)
        everyone(back)
        scale = tokens()
        reduce("q", qb, qr, qacc)
        gq[t, blk(j)] = (rkeep[:, :1] * qacc[...]).astype(BF)
        share("gq", gq, False)
        finish_output(scale)
        finish_value_arriving(scale)
        got("w", 0, w1o)
        drain_common()

        def rest(b):
            sent("a", b, src.at[0])
            sent("xf", b, xs.at[t, blk(b)])
        others(rest)

        def rest_all(b):
            sent("pjf", b, pj.at[t, blk(b)])
            sent("x", b, yx.at[blk(b)])
            sent("uf", b, us.at[t, blk(b)])
        everyone(rest_all)

    def middle_section():
        start_common()

        def chunk(b):
            arrive("x", "xf", xs, b)
            forward_chunk(b, False)
        everyone(chunk)
        forward_out()

        def back(b):
            arrive("g", "uf", us, b)
            backward_chunk(b)
        everyone(back)
        backward_out(False)
        scale = tokens()
        finish_output(scale)
        finish_value(scale)
        drain_common()
        sent("e", 0, exs)
        others(lambda b: sent("sc", b, sc.at[b]))

        def rest_all(b):
            sent("xf", b, xs.at[t, blk(b)])
            sent("uf", b, us.at[t, blk(b)])
            sent("pjf", b, pj.at[t, blk(b)])
            sent("gqf", b, gq.at[t, blk(b)])
            sent("x", b, yx.at[blk(b)])
            sent("g", b, yg.at[blk(b)])
        everyone(rest_all)

    def last_section():
        start_common()
        all_to_all(us)
        backward_chunk(j)
        row_info()

        def seeds(b):
            arrive("a", "uf", us, b)
            backward_chunk(b)
        others(seeds)

        def chunk(b):
            arrive("x", "xf", xs, b)
            forward_chunk(b, True)
        everyone(chunk)
        own_inverse()
        reduce("p", pb, pr, pacc)
        backward_out(True)
        share("pj", pj, False)
        scale = tokens()
        finish_value(scale)
        others(lambda b: got("pj", b, pj.at[t, blk(b)]))
        finish_output(scale)
        got("w", 1, w2o)
        drain_common()
        sent("e", 0, exs)

        def rest(b):
            sent("a", b, src.at[0])
            sent("uf", b, us.at[t, blk(b)])
            sent("sc", b, sc.at[b])
        others(rest)

        def rest_all(b):
            sent("xf", b, xs.at[t, blk(b)])
            sent("gqf", b, gq.at[t, blk(b)])
            sent("g", b, yg.at[blk(b)])
        everyone(rest_all)

    pl.when(s == 0)(first_section)
    pl.when(s == last)(last_section)
    if sections > 2:
        pl.when((s > 0) & (s < last))(middle_section)


def local(
    hidden, unembed, value_proj, output_proj, norm_gains, survive, lengths, assign,
    advantage, reference_logit, recorded_gap,
):
    n = lax.axis_size("dp")
    sections = lax.axis_size("section")
    s = lax.axis_index("section")
    count, positions, width = hidden.shape
    rows = count * positions
    part = value_proj.shape[1]
    half = part // 2
    v = value_proj.shape[2]

    src = jnp.where(s == sections - 1, unembed, hidden).reshape(rows, n * 2, half)
    src = src.transpose(1, 0, 2)
    w1 = value_proj[0].reshape(2, half, v)
    w2 = output_proj[0].reshape(v, 2, half).transpose(1, 0, 2)
    gains = norm_gains[0].reshape(n * 2, 1, half)
    total = n * rows
    kinds = len(KINDS)
    vm = pl.BlockSpec(memory_space=pltpu.VMEM)
    dw1, dw2 = pl.pallas_call(
        functools.partial(kernel, n, sections, width),
        out_shape=(
            jax.ShapeDtypeStruct((2, half, v), F32),
            jax.ShapeDtypeStruct((v, part), F32),
        ),
        in_specs=[vm] * 10,
        out_specs=(vm, vm),
        scratch_shapes=[
            pltpu.VMEM((2, total, half), BF),
            pltpu.VMEM((2, total, half), BF),
            pltpu.VMEM((2, total, half), BF),
            pltpu.VMEM((total, v), BF),
            pltpu.VMEM((n, rows, v), BF),
            pltpu.VMEM((total, v), BF),
            pltpu.VMEM((n, rows, v), BF),
            pltpu.VMEM((2, total, v), BF),
            pltpu.VMEM((2, total, v), BF),
            pltpu.VMEM((n, 8, rows), F32),
            pltpu.VMEM((half, v), BF),
            pltpu.VMEM((v, half), BF),
            pltpu.VMEM((total, half), BF),
            pltpu.VMEM((total, half), BF),
            pltpu.VMEM((n, 8, LANES), F32),
            pltpu.VMEM((rows, LANES), F32),
            pltpu.VMEM((rows, LANES), F32),
            pltpu.VMEM((rows, v), F32),
            pltpu.VMEM((rows, v), F32),
            pltpu.VMEM((rows, LANES), F32),
            pltpu.VMEM((n, 8, rows), F32),
            pltpu.VMEM((n, 8, rows), F32),
            pltpu.VMEM((rows, LANES), F32),
            pltpu.VMEM((8, LANES), F32),
            pltpu.SemaphoreType.DMA((kinds, n)),
            pltpu.SemaphoreType.DMA((kinds, n)),
        ],
        compiler_params=pltpu.CompilerParams(
            collective_id=0, has_side_effects=True, vmem_limit_bytes=60 * 1024 * 1024
        ),
    )(
        src, w1, w2, gains, survive.reshape(1, -1), lengths.reshape(1, count),
        assign.reshape(1, count), advantage.reshape(1, count), reference_logit.T, recorded_gap.T,
    )
    return (
        dw1.reshape(1, part, v),
        dw2[None],
    )


def solution(mesh):
    rowwise = P(("groups", "dp"))
    placed = (
        P(("groups", "dp"), None, None),
        P(("groups", "dp"), None, None),
        P("section", "dp", "tensor"),
        P("section", "tensor", "dp"),
        P("section", None),
        rowwise,
        rowwise,
        rowwise,
        rowwise,
        P(("groups", "dp"), None),
        P(("groups", "dp"), None),
    )
    return jax.shard_map(
        local,
        mesh=mesh,
        in_specs=placed,
        out_specs=(
            P(("groups", "section"), "dp", "tensor"),
            P(("groups", "section"), "tensor", "dp"),
        ),
        check_vma=False,
    )
```
